256 devices in a mesh: row: 8 (over y, z_hi), col: 32 (over x, z_lo, core).
Axes of the slice: x: 4, y: 4, z: 8 (z_hi: 2, z_lo: 4; z = z_hi * 4 + z_lo), core: 2. Of those that a mesh axis runs over, the one named last changes fastest.
Arguments:
- pair_grad: float32 [2048, 2048, 128], P('row', 'col'), may hold values from -4 to 4
- out_weight: bfloat16 [1024, 128], replicated, may hold values from -0.1875 to 0.1875
- left_factor: bfloat16 [32, 32, 2048], P('col', None, 'row'), may hold values from -6 to 6
- right_factor: bfloat16 [32, 32, 2048], P('row', None, 'col'), may hold values from -6 to 6
Outputs:
- left_grad: float32 [32, 32, 2048], P('col', None, 'row')
- right_grad: float32 [32, 32, 2048], P('row', None, 'col')
The draws below stay inside these ranges and needn't reach their ends.
All inputs are finite; a program needn't handle non-finite values.
Results may differ from the reference program's by a relative error of at most 0.0042.
Values may be sent and summed in bfloat16 or wider, within the bound.
A program may use at most 128 MiB of HBM per device.

```python
import math
import jax
import jax.numpy as jnp
from jax import lax

C = 32
P_SIZE = 128
S = 32
TOKENS = 2048


def levels(rng, dims, split, smallest, top_value):
    def one(position, parts):
        draws = jax.random.uniform(jax.random.fold_in(jax.random.fold_in(rng, 6), position), (parts,), jnp.float32, smallest / len(split), top_value / len(split))
        return jnp.repeat(jnp.exp(draws), dims[position] // parts).reshape((-1,) + (1,) * (len(dims) - position - 1))

    factor_of = one(*split[0])
    for cut in split[1:]:
        factor_of = factor_of * one(*cut)
    return factor_of


def noise(key, dims, deviation, reach, pieces=(), kind=jnp.bfloat16):
    loudness = levels(key, dims, pieces, -0.22, 0.18) if pieces else 1.0
    array = jax.random.normal(key, dims, jnp.float32) * deviation * loudness
    return jnp.minimum(jnp.maximum(array, -reach), reach).astype(kind)


def setup_inputs(seed: int = 0) -> dict:
    seeds = jax.random.split(jax.random.key(seed), 5)
    pair_grad = noise(seeds[0], (TOKENS, TOKENS, P_SIZE), 0.5, 4.0, ((0, 8), (1, 32)), jnp.float32)
    out_weight = noise(seeds[1], (C * C, P_SIZE), (C * C) ** -0.5, 0.1875)
    left_factor = noise(seeds[2], (S, C, TOKENS), 1.0, 6.0, ((0, 32), (2, 8)))
    right_factor = noise(seeds[3], (S, C, TOKENS), 1.0, 6.0, ((0, 8), (2, 32)))
    return dict(pair_grad=pair_grad, out_weight=out_weight, left_factor=left_factor, right_factor=right_factor)


def reference(pair_grad, out_weight, left_factor, right_factor):
    rows_per_block = math.gcd(TOKENS, 32)
    sequence_count = TOKENS // rows_per_block
    pair_low = pair_grad.astype(jnp.bfloat16)
    grid = out_weight.astype(jnp.float32).reshape(C, C, P_SIZE)
    left_wide = left_factor.astype(jnp.float32)
    right_wide = right_factor.astype(jnp.float32)

    def step(carry, index):
        start = (index * rows_per_block).astype(jnp.int32)
        block = lax.dynamic_slice_in_dim(pair_low, start, rows_per_block, 0).astype(jnp.float32)
        expanded = jnp.einsum("ijk,xyk->ijxy", block, grid).astype(jnp.bfloat16)
        expanded = lax.optimization_barrier(expanded).astype(jnp.float32)
        left_block = lax.dynamic_slice_in_dim(left_wide, start, rows_per_block, 2)
        left_portion = jnp.einsum("ijxy,syj->sxi", expanded, right_wide)
        carry = carry + jnp.einsum("ijxy,sxi->syj", expanded, left_block)
        return carry, left_portion

    initial_carry = jnp.zeros((S, C, TOKENS), jnp.float32)
    right_total, left_portions = lax.scan(step, initial_carry, jnp.arange(sequence_count, dtype=jnp.int32))
    left_total = jnp.transpose(left_portions, (1, 2, 0, 3)).reshape(S, C, TOKENS)
    return left_total * (1.0 / S), right_total * (1.0 / S)
```

```python
import jax
import jax.numpy as jnp
from jax import lax
from jax.experimental import pallas as pl
from jax.experimental.pallas import tpu as pltpu
from jax.sharding import PartitionSpec as P

f32, bf16 = jnp.float32, jnp.bfloat16
MESH = pl.DeviceIdType.MESH
NT = (((1,), (1,)), ((), ()))

I, J, K, X, Y, S = 256, 64, 128, 32, 32, 32
ROWS, COLS, CHIPS = 8, 32, 16
G = 4
JA = 16
SCALE = 1.0 / S


def kernel(
    pair, weight, left, right,
    left_out, right_out,
    pf, pb, abuf, ubuf,
    rmine, rin, rst, rbuf,
    lin, lst, lbuf,
    acc, lxs, lx, lsend, lr,
    rt, rsend, rr,
    psem, osem, rs_sem, rr_in, ls_sem, l_in, lrs_sem, lr_in,
    xs_sem, x_in, gs_sem, g_in, hs_sem, h_in,
):
    row, col = lax.axis_index("row"), lax.axis_index("col")
    y, zh = row // 2, row % 2
    chip, core = col // 2, col % 2
    mate = (row, chip * 2 + 1 - core)

    def row_peer(h, t):
        return ((y + t) % 4) * 2 + (zh + h) % 2

    def chip_peer(d):
        return ((chip + d) % CHIPS) * 2 + core

    def slot_of(s):
        owner, s4 = s // G, s % G
        return ((owner + zh) % 2) * 16 + (s4 % 2) * 8 + (s4 // 2) * 4 + (owner // 2 - y + 4) % 4

    mine = slot_of(col)

    own = pltpu.make_async_copy(left.at[0], lin.at[mine], osem)
    own.start()

    @pl.loop(0, I)
    def _(i):
        pltpu.make_async_copy(pair.at[i], pf.at[:, i, :], psem).start()

    barrier = pltpu.get_barrier_semaphore()
    for h in range(2):
        for t in range(4):
            if h or t:
                pl.semaphore_signal(barrier, inc=1, device_id=(row_peer(h, t), col), device_id_type=MESH)
    pl.semaphore_signal(barrier, inc=1, device_id=mate, device_id_type=MESH)

    @pl.loop(1, CHIPS)
    def _(d):
        pl.semaphore_signal(barrier, inc=1, device_id=(row, chip_peer(d)), device_id_type=MESH)

    flipped = jnp.transpose(right[...].reshape(G * Y, J).astype(f32)).astype(bf16)
    rmine[...] = flipped
    rin[0] = flipped
    own.wait()
    pl.semaphore_wait(barrier, ROWS - 1 + 1 + CHIPS - 1)

    def right_copy(h, t):
        return pltpu.make_async_remote_copy(
            rmine, rin.at[h * 4 + (4 - t) % 4], rs_sem, rr_in.at[h],
            device_id=(row_peer(h, t), col), device_id_type=MESH)

    for h in (1, 0):
        for t in range(4):
            if h or t:
                right_copy(h, t).start()

    @pl.loop(1, CHIPS)
    def _(d):
        pltpu.make_async_remote_copy(
            lin.at[mine], lin.at[mine], ls_sem, l_in,
            device_id=(row, chip_peer(d)), device_id_type=MESH).start()

    lane = lax.broadcasted_iota(jnp.int32, (4, 128), 1) // 32

    def spread_right(h):
        rst[pl.ds(4 * h, 4)] = rin[pl.ds(4 * h, 4)].astype(f32)

        @pl.loop(0, J // 4)
        def _(q):
            for e in range(4):
                v = rst[pl.ds(4 * h, 4), q * 4 + e, :]
                rows = [jnp.where(lane == s4, v, 0.0) for s4 in (0, 2, 1, 3)]
                rbuf[h, q * 4 + e] = jnp.concatenate(rows, axis=0).astype(bf16)

    def pair_of(x2):
        a = weight[pl.ds(64 * x2, 32), :]
        b = weight[pl.ds(64 * x2 + 32, 32), :]
        return jnp.concatenate([a, b], axis=1)

    def times_weight(h):
        @pl.loop(0, J // JA)
        def _(c):
            lhs = rbuf[h, pl.ds(c * JA, JA)].reshape(JA * 16, 128)
            for x2 in range(X // 2):
                rhs = jnp.concatenate([pair_of(x2)] * 4, axis=0)
                o = jnp.dot(lhs, rhs, preferred_element_type=f32).astype(bf16)
                for j in range(JA):
                    for e in range(2):
                        abuf[2 * x2 + e, :, pl.ds((c * JA + j) * K, K)] = (
                            o[j * 16 : j * 16 + 16, e * K : e * K + K])

    def left_sums(h):
        for c in range(J // JA):
            j0 = c * JA
            rhs = jnp.concatenate([pb[j0 + j] for j in range(JA)], axis=1)
            lhs = abuf[:, :, pl.ds(j0 * K, JA * K)].reshape(X * 16, JA * K)
            o = lax.dot_general(lhs, rhs, NT, preferred_element_type=f32)
            for e in range(2):
                v = o[:, e * 128 : e * 128 + 128].reshape(X, 16, 128)
                if c == 0:
                    acc[h, e, :, pl.ds(0, 16), :] = v
                else:
                    acc[h, e, :, pl.ds(0, 16), :] += v

    def left_block(h, n):
        v = [acc[h, e, :, n, :] for e in range(2)]
        return jnp.concatenate(v, axis=1) * SCALE

    def exchange(h):
        return pltpu.make_async_remote_copy(
            lxs.at[h], lx.at[h], xs_sem.at[h], x_in.at[h], device_id=mate, device_id_type=MESH)

    def give_mate(h):
        @pl.when(core == 0)
        def _():
            for n in range(8):
                lxs[h, n] = left_block(h, 8 + n).astype(bf16)

        @pl.when(core == 1)
        def _():
            for n in range(8):
                lxs[h, n] = left_block(h, n).astype(bf16)

        exchange(h).start()

    def left_copy(h, n):
        s = row_peer(h, n % 4) * G + (n // 4) * 2 + core
        there = s // 2
        return s, pltpu.make_async_remote_copy(
            lsend.at[h, n], lr.at[(chip - there + CHIPS) % CHIPS], gs_sem, g_in,
            device_id=(row, s), device_id_type=MESH)

    def send_left(h):
        exchange(h).wait_recv()

        @pl.when(core == 0)
        def _():
            for n in range(8):
                lsend[h, n] = (left_block(h, n) + lx[h, n].astype(f32)).astype(bf16)

        @pl.when(core == 1)
        def _():
            for n in range(8):
                lsend[h, n] = (left_block(h, 8 + n) + lx[h, n].astype(f32)).astype(bf16)

        for n in range(8):
            s, copy = left_copy(h, n)

            @pl.when(s != col)
            def _():
                copy.start()

            @pl.when(s == col)
            def _():
                lr[0] = lsend[h, n]

    def relay(h):
        part = lin.at[pl.ds(h * 16 + core * 8, 8)]
        return pltpu.make_async_remote_copy(
            part, part, lrs_sem.at[h], lr_in.at[h], device_id=mate, device_id_type=MESH)

    def spread_left(h):
        for e in range(2):
            lst[e, :, pl.ds(0, X), :] = lin[pl.ds(h * 16, 16), :, pl.ds(e * 128, 128)].astype(f32)

        @pl.loop(0, X // 4)
        def _(q):
            for d in range(4):
                x = q * 4 + d
                v = [lst[e, :, x, :] for e in range(2)]
                lbuf[h, x] = jnp.concatenate(v, axis=1).astype(bf16)

    def times_left(h):
        @pl.loop(0, J // JA)
        def _(c):
            lhs = lbuf[h].reshape(X * 16, I)
            for j2 in range(JA // 2):
                j = c * JA + 2 * j2
                rhs = jnp.concatenate([pb[j], pb[j + 1]], axis=1)
                o = jnp.dot(lhs, rhs, preferred_element_type=f32).astype(bf16)
                for e in range(2):
                    ubuf[:, j + e] = o[:, e * K : e * K + K].reshape(X, 16, K)

    def right_sums(h):
        @pl.loop(0, J // JA)
        def _(c):
            t = jnp.zeros((JA * 16, Y), f32)
            for x2 in range(X // 2):
                lhs = [ubuf[2 * x2 + e, pl.ds(c * JA, JA)].reshape(JA * 16, K) for e in range(2)]
                t = t + lax.dot_general(
                    jnp.concatenate(lhs, axis=1), pair_of(x2), NT, preferred_element_type=f32)
            rt[pl.ds(c * JA, JA), pl.ds(0, 16), :] = (t * SCALE).reshape(JA, 16, Y)

    def right_copy_back(h, t):
        return pltpu.make_async_remote_copy(
            rsend.at[h * 4 + t], rr.at[h * 4 + (4 - t) % 4], hs_sem, h_in.at[h],
            device_id=(row_peer(h, t), col), device_id_type=MESH)

    def send_right(h):
        for t in range(4):
            v = [rt[:, (s4 % 2) * 8 + (s4 // 2) * 4 + t, :] for s4 in range(G)]
            v = jnp.concatenate(v, axis=1).astype(bf16)
            if h or t:
                rsend[h * 4 + t] = v
                right_copy_back(h, t).start()
            else:
                rr[0] = v

    pltpu.make_async_copy(pf, pf, psem).wait()

    @pl.loop(0, J // 8)
    def _(c):
        pb[pl.ds(c * 8, 8)] = pf[pl.ds(c * 8, 8)].astype(bf16)

    pltpu.make_async_copy(rin.at[pl.ds(1, 3)], rin.at[pl.ds(1, 3)], rr_in.at[0]).wait()
    spread_right(0)
    times_weight(0)
    left_sums(0)
    give_mate(0)
    pltpu.make_async_copy(rin.at[pl.ds(4, 4)], rin.at[pl.ds(4, 4)], rr_in.at[1]).wait()
    spread_right(1)
    times_weight(1)
    send_left(0)
    pltpu.make_async_copy(lin.at[pl.ds(0, 15)], lin.at[pl.ds(0, 15)], l_in).wait()
    relay(0).start()
    relay(1).start()
    left_sums(1)
    give_mate(1)

    relay(1).wait_recv()
    spread_left(1)
    relay(0).wait_recv()
    spread_left(0)
    send_left(1)
    times_left(1)
    right_sums(1)
    send_right(1)
    times_left(0)
    right_sums(0)
    send_right(0)

    pltpu.make_async_copy(lr.at[pl.ds(1, 15)], lr.at[pl.ds(1, 15)], g_in).wait()
    total = lr[0].astype(f32)
    for d in range(1, CHIPS):
        total = total + lr[d].astype(f32)
    left_out[0] = total
    pltpu.make_async_copy(rr.at[pl.ds(4, 4)], rr.at[pl.ds(4, 4)], h_in.at[1]).wait()
    pltpu.make_async_copy(rr.at[pl.ds(1, 3)], rr.at[pl.ds(1, 3)], h_in.at[0]).wait()
    total = rr[0].astype(f32)
    for d in range(1, ROWS):
        total = total + rr[d].astype(f32)
    right_out[...] = jnp.transpose(total).reshape(G, Y, J)

    pltpu.make_async_copy(rin.at[pl.ds(0, 7)], rin.at[pl.ds(0, 7)], rs_sem).wait()
    pltpu.make_async_copy(lin.at[pl.ds(0, 15)], lin.at[pl.ds(0, 15)], ls_sem).wait()
    for h in range(2):
        relay(h).wait_send()
        exchange(h).wait_send()
    pltpu.make_async_copy(lr.at[pl.ds(0, 15)], lr.at[pl.ds(0, 15)], gs_sem).wait()
    pltpu.make_async_copy(rr.at[pl.ds(0, 7)], rr.at[pl.ds(0, 7)], hs_sem).wait()


def body(pair_grad, out_weight, left_factor, right_factor):
    vmem = pl.BlockSpec(memory_space=pltpu.VMEM)
    hbm = pl.BlockSpec(memory_space=pl.ANY)
    dma = pltpu.SemaphoreType.DMA
    return pl.pallas_call(
        kernel,
        out_shape=(
            jax.ShapeDtypeStruct((1, X, I), f32),
            jax.ShapeDtypeStruct((G, Y, J), f32),
        ),
        in_specs=[hbm, vmem, hbm, vmem],
        out_specs=(vmem, vmem),
        scratch_shapes=[
            pltpu.VMEM((J, I, K), f32),
            pltpu.VMEM((J, I, K), bf16),
            pltpu.VMEM((X, 16, J * K), bf16),
            pltpu.VMEM((X, J, 16, K), bf16),
            pltpu.VMEM((J, 128), bf16),
            pltpu.VMEM((ROWS, J, 128), bf16),
            pltpu.VMEM((ROWS, J, 128), f32),
            pltpu.VMEM((2, J, 16, 128), bf16),
            pltpu.VMEM((S, X, I), bf16),
            pltpu.VMEM((2, 16, 40, 128), f32),
            pltpu.VMEM((2, X, 16, I), bf16),
            pltpu.VMEM((2, 2, X, 24, 128), f32),
            pltpu.VMEM((2, 8, X, I), bf16),
            pltpu.VMEM((2, 8, X, I), bf16),
            pltpu.VMEM((2, 8, X, I), bf16),
            pltpu.VMEM((CHIPS, X, I), bf16),
            pltpu.VMEM((J, 24, Y), f32),
            pltpu.VMEM((ROWS, J, 128), bf16),
            pltpu.VMEM((ROWS, J, 128), bf16),
            dma, dma, dma, dma((2,)), dma, dma, dma((2,)), dma((2,)),
            dma((2,)), dma((2,)), dma, dma, dma, dma((2,)),
        ],
        compiler_params=pltpu.CompilerParams(
            collective_id=0, has_side_effects=True, vmem_limit_bytes=60 * 2**20),
        name="outer_product_mean_backward",
    )(pair_grad, out_weight, left_factor, right_factor)


def solution(mesh):
    placed = (P("row", "col", None), P(), P("col", None, "row"), P("row", None, "col"))
    return jax.shard_map(
        body,
        mesh=mesh,
        in_specs=placed,
        out_specs=(P("col", None, "row"), P("row", None, "col")),
        check_vma=False,
    )
```

```python
import jax
import jax.numpy as jnp
from jax import lax
from jax.experimental import pallas as pl
from jax.experimental.pallas import tpu as pltpu
from jax.sharding import PartitionSpec as P

f32, bf16 = jnp.float32, jnp.bfloat16
MESH = pl.DeviceIdType.MESH
NT = (((1,), (1,)), ((), ()))

I, J, K, X, Y, S = 256, 64, 128, 32, 32, 32
ROWS, COLS, CHIPS = 8, 32, 16
G = 4
JA, JB = 16, 32
SCALE = 1.0 / S
VMEM_LIMIT = 57 * 2**20


def kernel(
    pair, wsrc, left, rsrc,
    left_out, right_out,
    weight, right, pf, pb, buf,
    rmine, rin, rst, rbuf,
    lin, lst, lbuf,
    acc, lxs, lx, lsend, lr,
    rt, rsend, rr,
    left_sum, right_sum, done,
    psem, osem, wsem, rsem, rs_sem, rr_in, ls_sem, l_in, lrs_sem, lr_in,
    xs_sem, x_in, gs_sem, g_in, hs_sem, h_in,
):
    row, col = lax.axis_index("row"), lax.axis_index("col")
    y, zh = row // 2, row % 2
    chip, core = col // 2, col % 2
    mate = (row, chip * 2 + 1 - core)

    def row_peer(h, t):
        return ((y + t) % 4) * 2 + (zh + h) % 2

    def chip_peer(d):
        return ((chip + d) % CHIPS) * 2 + core

    def slot_of(s):
        owner, s4 = s // G, s % G
        return ((owner + zh) % 2) * 16 + (s4 % 2) * 8 + (s4 // 2) * 4 + (owner // 2 - y + 4) % 4

    mine = slot_of(col)

    barrier = pltpu.get_barrier_semaphore()
    for h in (1, 0):
        for t in range(4):
            if h or t:
                pl.semaphore_signal(barrier, inc=1, device_id=(row_peer(h, t), col), device_id_type=MESH)
    pl.semaphore_signal(barrier, inc=1, device_id=mate, device_id_type=MESH)

    @pl.loop(1, CHIPS)
    def _(d):
        pl.semaphore_signal(barrier, inc=1, device_id=(row, chip_peer(d)), device_id_type=MESH)

    own = pltpu.make_async_copy(left.at[0], lin.at[mine], osem)
    own.start()
    rload = pltpu.make_async_copy(rsrc, right, rsem)
    rload.start()
    wload = pltpu.make_async_copy(wsrc, weight, wsem)
    wload.start()

    @pl.loop(0, I)
    def _(i):
        pltpu.make_async_copy(pair.at[i], pf.at[:, i, :], psem).start()

    rload.wait()
    flipped = jnp.transpose(right[...].reshape(G * Y, J).astype(f32)).astype(bf16)
    rmine[...] = flipped
    rin[0] = flipped
    own.wait()
    pl.semaphore_wait(barrier, ROWS - 1 + 1 + CHIPS - 1)

    def right_copy(h, t):
        return pltpu.make_async_remote_copy(
            rmine, rin.at[h * 4 + (4 - t) % 4], rs_sem, rr_in.at[h],
            device_id=(row_peer(h, t), col), device_id_type=MESH)

    for h in (1, 0):
        for t in range(4):
            if h or t:
                right_copy(h, t).start()

    @pl.loop(1, CHIPS)
    def _(d):
        pltpu.make_async_remote_copy(
            lin.at[mine], lin.at[mine], ls_sem, l_in,
            device_id=(row, chip_peer(d)), device_id_type=MESH).start()

    lane = lax.broadcasted_iota(jnp.int32, (4, 128), 1) // 32

    def spread_right(h):
        rst[pl.ds(4 * h, 4)] = rin[pl.ds(4 * h, 4)].astype(f32)

        @pl.loop(0, J // 4)
        def _(q):
            for e in range(4):
                v = rst[pl.ds(4 * h, 4), q * 4 + e, :]
                rows = [jnp.where(lane == s4, v, 0.0) for s4 in (0, 2, 1, 3)]
                rbuf[h, q * 4 + e] = jnp.concatenate(rows, axis=0).astype(bf16)

    def pair_of(x2):
        a = weight[pl.ds(64 * x2, 32), :]
        b = weight[pl.ds(64 * x2 + 32, 32), :]
        return jnp.concatenate([a, b], axis=1)

    def times_weight(h):
        @pl.loop(0, J // JB)
        def _(c):
            lhs = rbuf[h, pl.ds(c * JB, JB)].reshape(JB * 16, 128)
            for x2 in range(X // 2):
                rhs = jnp.concatenate([pair_of(x2)] * 4, axis=0)
                o = jnp.dot(lhs, rhs, preferred_element_type=f32).astype(bf16)
                for j in range(JB):
                    for e in range(2):
                        buf[2 * x2 + e, c * JB + j] = o[j * 16 : j * 16 + 16, e * K : e * K + K]

    def left_sums(h):
        rhs = jnp.concatenate([pb[j] for j in range(J)], axis=1)
        lhs = jnp.concatenate([buf[:, j].reshape(X * 16, K) for j in range(J)], axis=1)
        o = lax.dot_general(lhs, rhs, NT, preferred_element_type=f32)
        for e in range(2):
            acc[h, e, :, pl.ds(0, 16), :] = o[:, e * 128 : e * 128 + 128].reshape(X, 16, 128)

    def left_block(h, n):
        v = [acc[h, e, :, n, :] for e in range(2)]
        return jnp.concatenate(v, axis=1) * SCALE

    def exchange(h):
        return pltpu.make_async_remote_copy(
            lxs.at[h], lx.at[h], xs_sem.at[h], x_in.at[h], device_id=mate, device_id_type=MESH)

    def give_mate(h):
        @pl.when(core == 0)
        def _():
            for n in range(8):
                lxs[h, n] = left_block(h, 8 + n).astype(bf16)

        @pl.when(core == 1)
        def _():
            for n in range(8):
                lxs[h, n] = left_block(h, n).astype(bf16)

        exchange(h).start()

    def left_copy(h, n):
        s = row_peer(h, n % 4) * G + (n // 4) * 2 + core
        there = s // 2
        return s, pltpu.make_async_remote_copy(
            lsend.at[h, n], lr.at[(chip - there + CHIPS) % CHIPS], gs_sem, g_in,
            device_id=(row, s), device_id_type=MESH)

    def send_left(h):
        exchange(h).wait_recv()

        @pl.when(core == 0)
        def _():
            for n in range(8):
                lsend[h, n] = (left_block(h, n) + lx[h, n].astype(f32)).astype(bf16)

        @pl.when(core == 1)
        def _():
            for n in range(8):
                lsend[h, n] = (left_block(h, 8 + n) + lx[h, n].astype(f32)).astype(bf16)

        for n in range(8):
            s, copy = left_copy(h, n)

            @pl.when(s != col)
            def _():
                copy.start()

            @pl.when(s == col)
            def _():
                lr[0] = lsend[h, n]

    def relay(h):
        part = lin.at[pl.ds(h * 16 + core * 8, 8)]
        return pltpu.make_async_remote_copy(
            part, part, lrs_sem.at[h], lr_in.at[h], device_id=mate, device_id_type=MESH)

    def spread_left(h):
        for e in range(2):
            lst[e, :, pl.ds(0, X), :] = lin[pl.ds(h * 16, 16), :, pl.ds(e * 128, 128)].astype(f32)

        @pl.loop(0, X // 4)
        def _(q):
            for d in range(4):
                x = q * 4 + d
                v = [lst[e, :, x, :] for e in range(2)]
                lbuf[h, x] = jnp.concatenate(v, axis=1).astype(bf16)

    def times_left(h):
        @pl.loop(0, J // JB)
        def _(c):
            lhs = lbuf[h].reshape(X * 16, I)
            for j2 in range(JB // 2):
                j = c * JB + 2 * j2
                rhs = jnp.concatenate([pb[j], pb[j + 1]], axis=1)
                o = jnp.dot(lhs, rhs, preferred_element_type=f32).astype(bf16)
                for e in range(2):
                    buf[:, j + e] = o[:, e * K : e * K + K].reshape(X, 16, K)

    def right_sums(h):
        for c in range(J // JA):
            t = jnp.zeros((JA * 16, Y), f32)
            for x2 in range(X // 2):
                lhs = [buf[2 * x2 + e, pl.ds(c * JA, JA)].reshape(JA * 16, K) for e in range(2)]
                t = t + lax.dot_general(
                    jnp.concatenate(lhs, axis=1), pair_of(x2), NT, preferred_element_type=f32)
            rt[pl.ds(c * JA, JA), pl.ds(0, 16), :] = (t * SCALE).reshape(JA, 16, Y)

    def right_copy_back(h, t):
        return pltpu.make_async_remote_copy(
            rsend.at[h * 4 + t], rr.at[h * 4 + (4 - t) % 4], hs_sem, h_in.at[h],
            device_id=(row_peer(h, t), col), device_id_type=MESH)

    def send_right(h):
        for t in range(4):
            v = [rt[:, (s4 % 2) * 8 + (s4 // 2) * 4 + t, :] for s4 in range(G)]
            v = jnp.concatenate(v, axis=1).astype(bf16)
            if h or t:
                rsend[h * 4 + t] = v
                right_copy_back(h, t).start()
            else:
                rr[0] = v

    wload.wait()
    pltpu.make_async_copy(pf, pf, psem).wait()

    @pl.loop(0, J // 8)
    def _(c):
        pb[pl.ds(c * 8, 8)] = pf[pl.ds(c * 8, 8)].astype(bf16)

    pltpu.make_async_copy(rin.at[pl.ds(1, 3)], rin.at[pl.ds(1, 3)], rr_in.at[0]).wait()
    spread_right(0)
    times_weight(0)
    left_sums(0)
    give_mate(0)
    pltpu.make_async_copy(rin.at[pl.ds(4, 4)], rin.at[pl.ds(4, 4)], rr_in.at[1]).wait()
    spread_right(1)
    times_weight(1)
    send_left(0)
    pltpu.make_async_copy(lin.at[pl.ds(0, 15)], lin.at[pl.ds(0, 15)], l_in).wait()
    relay(0).start()
    relay(1).start()
    left_sums(1)
    give_mate(1)

    relay(1).wait_recv()
    spread_left(1)
    relay(0).wait_recv()
    spread_left(0)
    send_left(1)
    times_left(1)
    right_sums(1)
    send_right(1)
    times_left(0)
    right_sums(0)
    send_right(0)

    pltpu.make_async_copy(lr.at[pl.ds(1, 15)], lr.at[pl.ds(1, 15)], g_in).wait()
    total = lr[0].astype(f32)
    for d in range(1, CHIPS):
        total = total + lr[d].astype(f32)
    left_sum[0] = total
    left_done = pltpu.make_async_copy(left_sum, left_out, done.at[0])
    left_done.start()
    pltpu.make_async_copy(rr.at[pl.ds(4, 4)], rr.at[pl.ds(4, 4)], h_in.at[1]).wait()
    pltpu.make_async_copy(rr.at[pl.ds(1, 3)], rr.at[pl.ds(1, 3)], h_in.at[0]).wait()
    total = rr[0].astype(f32)
    for d in range(1, ROWS):
        total = total + rr[d].astype(f32)
    right_sum[...] = jnp.transpose(total).reshape(G, Y, J)
    right_done = pltpu.make_async_copy(right_sum, right_out, done.at[1])
    right_done.start()

    pltpu.make_async_copy(rin.at[pl.ds(0, 7)], rin.at[pl.ds(0, 7)], rs_sem).wait()
    pltpu.make_async_copy(lin.at[pl.ds(0, 15)], lin.at[pl.ds(0, 15)], ls_sem).wait()
    for h in range(2):
        relay(h).wait_send()
        exchange(h).wait_send()
    pltpu.make_async_copy(lr.at[pl.ds(0, 15)], lr.at[pl.ds(0, 15)], gs_sem).wait()
    pltpu.make_async_copy(rr.at[pl.ds(0, 7)], rr.at[pl.ds(0, 7)], hs_sem).wait()
    left_done.wait()
    right_done.wait()


def hand_over(left, right, left_out, right_out, left_in, right_in, sem):
    loads = [
        pltpu.make_async_copy(left, left_in, sem.at[0]),
        pltpu.make_async_copy(right, right_in, sem.at[1]),
    ]
    stores = [
        pltpu.make_async_copy(left_in, left_out, sem.at[2]),
        pltpu.make_async_copy(right_in, right_out, sem.at[3]),
    ]
    for load in loads:
        load.start()
    for load, store in zip(loads, stores):
        load.wait()
        store.start()
    for store in stores:
        store.wait()


def body(pair_grad, out_weight, left_factor, right_factor):
    hbm = pl.BlockSpec(memory_space=pltpu.HBM)
    dma = pltpu.SemaphoreType.DMA
    sums = pl.pallas_call(
        kernel,
        out_shape=(
            jax.ShapeDtypeStruct((1, X, I), f32),
            jax.ShapeDtypeStruct((G, Y, J), f32),
        ),
        in_specs=[hbm] * 4,
        out_specs=(hbm, hbm),
        scratch_shapes=[
            pltpu.VMEM((X * Y, K), bf16),
            pltpu.VMEM((G, Y, J), bf16),
            pltpu.VMEM((J, I, K), f32),
            pltpu.VMEM((J, I, K), bf16),
            pltpu.VMEM((X, J, 16, K), bf16),
            pltpu.VMEM((J, 128), bf16),
            pltpu.VMEM((ROWS, J, 128), bf16),
            pltpu.VMEM((ROWS, J, 128), f32),
            pltpu.VMEM((2, J, 16, 128), bf16),
            pltpu.VMEM((S, X, I), bf16),
            pltpu.VMEM((2, 16, 40, 128), f32),
            pltpu.VMEM((2, X, 16, I), bf16),
            pltpu.VMEM((2, 2, X, 24, 128), f32),
            pltpu.VMEM((2, 8, X, I), bf16),
            pltpu.VMEM((2, 8, X, I), bf16),
            pltpu.VMEM((2, 8, X, I), bf16),
            pltpu.VMEM((CHIPS, X, I), bf16),
            pltpu.VMEM((J, 24, Y), f32),
            pltpu.VMEM((ROWS, J, 128), bf16),
            pltpu.VMEM((ROWS, J, 128), bf16),
            pltpu.VMEM((1, X, I), f32),
            pltpu.VMEM((G, Y, J), f32),
            dma((2,)),
            dma, dma, dma, dma, dma, dma((2,)), dma, dma, dma((2,)), dma((2,)),
            dma((2,)), dma((2,)), dma, dma, dma, dma((2,)),
        ],
        compiler_params=pltpu.CompilerParams(
            collective_id=0, has_side_effects=True, vmem_limit_bytes=VMEM_LIMIT),
        name="outer_product_mean_backward",
    )(pair_grad, out_weight, left_factor, right_factor)
    return pl.pallas_call(
        hand_over,
        out_shape=(
            jax.ShapeDtypeStruct((1, X, I), f32),
            jax.ShapeDtypeStruct((G, Y, J), f32),
        ),
        in_specs=[hbm, hbm],
        out_specs=(hbm, hbm),
        scratch_shapes=[
            pltpu.VMEM((1, X, I), f32),
            pltpu.VMEM((G, Y, J), f32),
            dma((4,)),
        ],
        name="hand_over",
    )(*sums)


def solution(mesh):
    placed = (P("row", "col", None), P(), P("col", None, "row"), P("row", None, "col"))
    return jax.shard_map(
        body,
        mesh=mesh,
        in_specs=placed,
        out_specs=(P("col", None, "row"), P("row", None, "col")),
        check_vma=False,
    )
```

```python
import jax
import jax.numpy as jnp
from jax import lax
from jax.experimental import pallas as pl
from jax.experimental.pallas import tpu as pltpu
from jax.sharding import PartitionSpec as P

f32, bf16 = jnp.float32, jnp.bfloat16
MESH = pl.DeviceIdType.MESH
NT = (((1,), (1,)), ((), ()))

I, J, K, X, Y, S = 256, 64, 128, 32, 32, 32
ROWS, COLS, CHIPS = 8, 32, 16
G = 4
JA, JB = 16, 32
SCALE = 1.0 / S
VMEM_LIMIT = 57 * 2**20


def kernel(
    pair, wsrc, left, rsrc,
    left_out, right_out,
    weight, right, pf, pb, buf,
    rmine, rin, rst, rbuf,
    lin, lst, lbuf,
    acc, lxs, lx, lsend, lr,
    rt, rsend, rr,
    left_sum, right_sum, done,
    psem, osem, wsem, rsem, rs_sem, rr_in, ls_sem, l_in, lrs_sem, lr_in,
    xs_sem, x_in, gs_sem, g_in, hs_sem, h_in,
):
    row, col = lax.axis_index("row"), lax.axis_index("col")
    y, zh = row // 2, row % 2
    chip, core = col // 2, col % 2
    mate = (row, chip * 2 + 1 - core)

    def row_peer(h, t):
        return ((y + t) % 4) * 2 + (zh + h) % 2

    def chip_peer(d):
        return ((chip + d) % CHIPS) * 2 + core

    def slot_of(s):
        owner, s4 = s // G, s % G
        return ((owner + zh) % 2) * 16 + (s4 % 2) * 8 + (s4 // 2) * 4 + (owner // 2 - y + 4) % 4

    mine = slot_of(col)

    barrier = pltpu.get_barrier_semaphore()
    for h in (1, 0):
        for t in range(4):
            if h or t:
                pl.semaphore_signal(barrier, inc=1, device_id=(row_peer(h, t), col), device_id_type=MESH)
    pl.semaphore_signal(barrier, inc=1, device_id=mate, device_id_type=MESH)

    @pl.loop(1, CHIPS)
    def _(d):
        pl.semaphore_signal(barrier, inc=1, device_id=(row, chip_peer(d)), device_id_type=MESH)

    own = pltpu.make_async_copy(left.at[0], lin.at[mine], osem)
    own.start()
    rload = pltpu.make_async_copy(rsrc, right, rsem)
    rload.start()
    wload = pltpu.make_async_copy(wsrc, weight, wsem)
    wload.start()

    @pl.loop(0, I)
    def _(i):
        pltpu.make_async_copy(pair.at[i], pf.at[:, i, :], psem).start()

    rload.wait()
    flipped = jnp.transpose(right[...].reshape(G * Y, J).astype(f32)).astype(bf16)
    rmine[...] = flipped
    rin[0] = flipped
    own.wait()
    pl.semaphore_wait(barrier, ROWS - 1 + 1 + CHIPS - 1)

    def right_copy(h, t):
        return pltpu.make_async_remote_copy(
            rmine, rin.at[h * 4 + (4 - t) % 4], rs_sem, rr_in.at[h],
            device_id=(row_peer(h, t), col), device_id_type=MESH)

    for h in (0, 1):
        for t in range(4):
            if h or t:
                right_copy(h, t).start()

    @pl.loop(1, CHIPS)
    def _(d):
        pltpu.make_async_remote_copy(
            lin.at[mine], lin.at[mine], ls_sem, l_in,
            device_id=(row, chip_peer(d)), device_id_type=MESH).start()

    lane = lax.broadcasted_iota(jnp.int32, (4, 128), 1) // 32

    def spread_right(h):
        rst[pl.ds(4 * h, 4)] = rin[pl.ds(4 * h, 4)].astype(f32)

        @pl.loop(0, J // 4)
        def _(q):
            for e in range(4):
                v = rst[pl.ds(4 * h, 4), q * 4 + e, :]
                rows = [jnp.where(lane == s4, v, 0.0) for s4 in (0, 2, 1, 3)]
                rbuf[h, q * 4 + e] = jnp.concatenate(rows, axis=0).astype(bf16)

    def pair_of(x2):
        a = weight[pl.ds(64 * x2, 32), :]
        b = weight[pl.ds(64 * x2 + 32, 32), :]
        return jnp.concatenate([a, b], axis=1)

    def times_weight(h):
        @pl.loop(0, J // JB)
        def _(c):
            lhs = rbuf[h, pl.ds(c * JB, JB)].reshape(JB * 16, 128)
            for x2 in range(X // 2):
                rhs = jnp.concatenate([pair_of(x2)] * 4, axis=0)
                o = jnp.dot(lhs, rhs, preferred_element_type=f32).astype(bf16)
                for j in range(JB):
                    for e in range(2):
                        buf[2 * x2 + e, c * JB + j] = o[j * 16 : j * 16 + 16, e * K : e * K + K]

    def left_sums(h):
        rhs = jnp.concatenate([pb[j] for j in range(J)], axis=1)
        lhs = jnp.concatenate([buf[:, j].reshape(X * 16, K) for j in range(J)], axis=1)
        o = lax.dot_general(lhs, rhs, NT, preferred_element_type=f32)
        for e in range(2):
            acc[h, e, :, pl.ds(0, 16), :] = o[:, e * 128 : e * 128 + 128].reshape(X, 16, 128)

    def left_block(h, n):
        v = [acc[h, e, :, n, :] for e in range(2)]
        return jnp.concatenate(v, axis=1) * SCALE

    def exchange(h):
        return pltpu.make_async_remote_copy(
            lxs.at[h], lx.at[h], xs_sem.at[h], x_in.at[h], device_id=mate, device_id_type=MESH)

    def give_mate(h):
        @pl.when(core == 0)
        def _():
            for n in range(8):
                lxs[h, n] = left_block(h, 8 + n).astype(bf16)

        @pl.when(core == 1)
        def _():
            for n in range(8):
                lxs[h, n] = left_block(h, n).astype(bf16)

        exchange(h).start()

    def left_copy(h, n):
        s = row_peer(h, n % 4) * G + (n // 4) * 2 + core
        there = s // 2
        return s, pltpu.make_async_remote_copy(
            lsend.at[h, n], lr.at[(chip - there + CHIPS) % CHIPS], gs_sem, g_in,
            device_id=(row, s), device_id_type=MESH)

    def send_left(h):
        exchange(h).wait_recv()

        @pl.when(core == 0)
        def _():
            for n in range(8):
                lsend[h, n] = (left_block(h, n) + lx[h, n].astype(f32)).astype(bf16)

        @pl.when(core == 1)
        def _():
            for n in range(8):
                lsend[h, n] = (left_block(h, 8 + n) + lx[h, n].astype(f32)).astype(bf16)

        for n in range(8):
            s, copy = left_copy(h, n)

            @pl.when(s != col)
            def _():
                copy.start()

            @pl.when(s == col)
            def _():
                lr[0] = lsend[h, n]

    def relay(h):
        part = lin.at[pl.ds(h * 16 + core * 8, 8)]
        return pltpu.make_async_remote_copy(
            part, part, lrs_sem.at[h], lr_in.at[h], device_id=mate, device_id_type=MESH)

    def spread_left(h):
        for e in range(2):
            lst[e, :, pl.ds(0, X), :] = lin[pl.ds(h * 16, 16), :, pl.ds(e * 128, 128)].astype(f32)

        @pl.loop(0, X // 4)
        def _(q):
            for d in range(4):
                x = q * 4 + d
                v = [lst[e, :, x, :] for e in range(2)]
                lbuf[h, x] = jnp.concatenate(v, axis=1).astype(bf16)

    def times_left(h):
        @pl.loop(0, J // JB)
        def _(c):
            lhs = lbuf[h].reshape(X * 16, I)
            for j2 in range(JB // 2):
                j = c * JB + 2 * j2
                rhs = jnp.concatenate([pb[j], pb[j + 1]], axis=1)
                o = jnp.dot(lhs, rhs, preferred_element_type=f32).astype(bf16)
                for e in range(2):
                    buf[:, j + e] = o[:, e * K : e * K + K].reshape(X, 16, K)

    def right_sums(h):
        for c in range(J // JA):
            t = jnp.zeros((JA * 16, Y), f32)
            for x2 in range(X // 2):
                lhs = [buf[2 * x2 + e, pl.ds(c * JA, JA)].reshape(JA * 16, K) for e in range(2)]
                t = t + lax.dot_general(
                    jnp.concatenate(lhs, axis=1), pair_of(x2), NT, preferred_element_type=f32)
            rt[pl.ds(c * JA, JA), pl.ds(0, 16), :] = (t * SCALE).reshape(JA, 16, Y)

    def right_copy_back(h, t):
        return pltpu.make_async_remote_copy(
            rsend.at[h * 4 + t], rr.at[h * 4 + (4 - t) % 4], hs_sem, h_in.at[h],
            device_id=(row_peer(h, t), col), device_id_type=MESH)

    def send_right(h):
        for t in range(4):
            v = [rt[:, (s4 % 2) * 8 + (s4 // 2) * 4 + t, :] for s4 in range(G)]
            v = jnp.concatenate(v, axis=1).astype(bf16)
            if h or t:
                rsend[h * 4 + t] = v
                right_copy_back(h, t).start()
            else:
                rr[0] = v

    wload.wait()
    pltpu.make_async_copy(pf, pf, psem).wait()

    @pl.loop(0, J // 8)
    def _(c):
        pb[pl.ds(c * 8, 8)] = pf[pl.ds(c * 8, 8)].astype(bf16)

    pltpu.make_async_copy(rin.at[pl.ds(1, 3)], rin.at[pl.ds(1, 3)], rr_in.at[0]).wait()
    spread_right(0)
    times_weight(0)
    left_sums(0)
    give_mate(0)
    pltpu.make_async_copy(rin.at[pl.ds(4, 4)], rin.at[pl.ds(4, 4)], rr_in.at[1]).wait()
    spread_right(1)
    times_weight(1)
    pltpu.make_async_copy(lin.at[pl.ds(0, 15)], lin.at[pl.ds(0, 15)], l_in).wait()
    relay(1).start()
    relay(0).start()
    send_left(0)
    left_sums(1)
    give_mate(1)

    relay(1).wait_recv()
    spread_left(1)
    relay(0).wait_recv()
    spread_left(0)
    send_left(1)
    times_left(1)
    right_sums(1)
    send_right(1)
    times_left(0)
    right_sums(0)
    send_right(0)

    pltpu.make_async_copy(lr.at[pl.ds(1, 15)], lr.at[pl.ds(1, 15)], g_in).wait()
    total = lr[0].astype(f32)
    for d in range(1, CHIPS):
        total = total + lr[d].astype(f32)
    left_sum[0] = total
    left_done = pltpu.make_async_copy(left_sum, left_out, done.at[0])
    left_done.start()
    pltpu.make_async_copy(rr.at[pl.ds(4, 4)], rr.at[pl.ds(4, 4)], h_in.at[1]).wait()
    pltpu.make_async_copy(rr.at[pl.ds(1, 3)], rr.at[pl.ds(1, 3)], h_in.at[0]).wait()
    total = rr[0].astype(f32)
    for d in range(1, ROWS):
        total = total + rr[d].astype(f32)
    right_sum[...] = jnp.transpose(total).reshape(G, Y, J)
    right_done = pltpu.make_async_copy(right_sum, right_out, done.at[1])
    right_done.start()

    pltpu.make_async_copy(rin.at[pl.ds(0, 7)], rin.at[pl.ds(0, 7)], rs_sem).wait()
    pltpu.make_async_copy(lin.at[pl.ds(0, 15)], lin.at[pl.ds(0, 15)], ls_sem).wait()
    for h in range(2):
        relay(h).wait_send()
        exchange(h).wait_send()
    pltpu.make_async_copy(lr.at[pl.ds(0, 15)], lr.at[pl.ds(0, 15)], gs_sem).wait()
    pltpu.make_async_copy(rr.at[pl.ds(0, 7)], rr.at[pl.ds(0, 7)], hs_sem).wait()
    left_done.wait()
    right_done.wait()


def hand_over(left, right, left_out, right_out, left_in, right_in, sem):
    loads = [
        pltpu.make_async_copy(left, left_in, sem.at[0]),
        pltpu.make_async_copy(right, right_in, sem.at[1]),
    ]
    stores = [
        pltpu.make_async_copy(left_in, left_out, sem.at[2]),
        pltpu.make_async_copy(right_in, right_out, sem.at[3]),
    ]
    for load in loads:
        load.start()
    for load, store in zip(loads, stores):
        load.wait()
        store.start()
    for store in stores:
        store.wait()


def body(pair_grad, out_weight, left_factor, right_factor):
    hbm = pl.BlockSpec(memory_space=pltpu.HBM)
    dma = pltpu.SemaphoreType.DMA
    sums = pl.pallas_call(
        kernel,
        out_shape=(
            jax.ShapeDtypeStruct((1, X, I), f32),
            jax.ShapeDtypeStruct((G, Y, J), f32),
        ),
        in_specs=[hbm] * 4,
        out_specs=(hbm, hbm),
        scratch_shapes=[
            pltpu.VMEM((X * Y, K), bf16),
            pltpu.VMEM((G, Y, J), bf16),
            pltpu.VMEM((J, I, K), f32),
            pltpu.VMEM((J, I, K), bf16),
            pltpu.VMEM((X, J, 16, K), bf16),
            pltpu.VMEM((J, 128), bf16),
            pltpu.VMEM((ROWS, J, 128), bf16),
            pltpu.VMEM((ROWS, J, 128), f32),
            pltpu.VMEM((2, J, 16, 128), bf16),
            pltpu.VMEM((S, X, I), bf16),
            pltpu.VMEM((2, 16, 40, 128), f32),
            pltpu.VMEM((2, X, 16, I), bf16),
            pltpu.VMEM((2, 2, X, 24, 128), f32),
            pltpu.VMEM((2, 8, X, I), bf16),
            pltpu.VMEM((2, 8, X, I), bf16),
            pltpu.VMEM((2, 8, X, I), bf16),
            pltpu.VMEM((CHIPS, X, I), bf16),
            pltpu.VMEM((J, 24, Y), f32),
            pltpu.VMEM((ROWS, J, 128), bf16),
            pltpu.VMEM((ROWS, J, 128), bf16),
            pltpu.VMEM((1, X, I), f32),
            pltpu.VMEM((G, Y, J), f32),
            dma((2,)),
            dma, dma, dma, dma, dma, dma((2,)), dma, dma, dma((2,)), dma((2,)),
            dma((2,)), dma((2,)), dma, dma, dma, dma((2,)),
        ],
        compiler_params=pltpu.CompilerParams(
            collective_id=0, has_side_effects=True, vmem_limit_bytes=VMEM_LIMIT),
        name="outer_product_mean_backward",
    )(pair_grad, out_weight, left_factor, right_factor)
    return pl.pallas_call(
        hand_over,
        out_shape=(
            jax.ShapeDtypeStruct((1, X, I), f32),
            jax.ShapeDtypeStruct((G, Y, J), f32),
        ),
        in_specs=[hbm, hbm],
        out_specs=(hbm, hbm),
        scratch_shapes=[
            pltpu.VMEM((1, X, I), f32),
            pltpu.VMEM((G, Y, J), f32),
            dma((4,)),
        ],
        name="hand_over",
    )(*sums)


def solution(mesh):
    placed = (P("row", "col", None), P(), P("col", None, "row"), P("row", None, "col"))
    return jax.shard_map(
        body,
        mesh=mesh,
        in_specs=placed,
        out_specs=(P("col", None, "row"), P("row", None, "col")),
        check_vma=False,
    )
```
